512 devices in a mesh: dp: 32 (over y, x, core), tp: 16 (over z).
Axes of the slice: x: 4, y: 4, z: 16, core: 2. Of those that a mesh axis runs over, the one named last changes fastest.
Arguments:
- slope_up: float32 [32, 1280, 5120], P('dp', None, 'tp'), may hold values from -1.25 to 1.25
- slope_down: float32 [32, 5120, 1280], P('dp', 'tp'), may hold values from -1.25 to 1.25
- slope_norm: float32 [32, 1280], P('dp'), may hold values from -12 to 12
- slope_bias: float32 [32, 1280], P('dp'), may hold values from -12 to 12
- param_up: float32 [1280, 5120], P('dp', 'tp'), may hold values from -0.15625 to 0.15625
- param_down: float32 [5120, 1280], P('tp', 'dp'), may hold values from -0.078125 to 0.078125
- param_norm: float32 [1280], P('dp'), may hold values from 0.25 to 1.75
- param_bias: float32 [1280], P('dp'), may hold values from -3 to 3
- state_up: float32 [1280, 5120], P('dp', 'tp'), may hold values from -1.75 to 1.75
- state_down: float32 [5120, 1280], P('tp', 'dp'), may hold values from -1.75 to 1.75
- state_norm: float32 [1280], P('dp'), may hold values from -1.75 to 1.75
- state_bias: float32 [1280], P('dp'), may hold values from -1.75 to 1.75
Outputs:
- half_up: bfloat16 [1280, 5120], P(None, 'tp')
- half_down: bfloat16 [5120, 1280], P('tp')
- half_norm: bfloat16 [1280], replicated
- half_bias: bfloat16 [1280], replicated
- next_up: float32 [1280, 5120], P('dp', 'tp')
- next_down: float32 [5120, 1280], P('tp', 'dp')
- next_norm: float32 [1280], P('dp')
- next_bias: float32 [1280], P('dp')
- state_new_up: float32 [1280, 5120], P('dp', 'tp')
- state_new_down: float32 [5120, 1280], P('tp', 'dp')
- state_new_norm: float32 [1280], P('dp')
- state_new_bias: float32 [1280], P('dp')
The draws below stay inside these ranges and needn't reach their ends.
All inputs are finite; a program needn't handle non-finite values.
Results may differ from the reference program's by a relative error of at most 0.009.
Values may be sent and summed in bfloat16 or wider, within the bound.
No kernel may reach another device: no remote copies, remote signals or barrier semaphores. Data moves between devices by JAX's collectives and lax.ppermute only.
A program may use at most 64 MiB of HBM per device.

```python
import jax
import jax.numpy as jnp

WIDTH = 1280
INNER = 5120
REPLICAS = 32


def strengthened(values, rng, source, target, parts, factor):
    owner, partner = [(jnp.arange(values.shape[position]) // (values.shape[position] // parts)).reshape([-1 if axis == position else 1 for axis in range(values.ndim)]) for position in (source, target)]
    chosen = jax.random.permutation(rng, parts)[partner]
    strong = (owner == chosen) | (owner == (partner + parts // 2) % parts)
    return jnp.where(strong, factor * values, values)


def shard_levels(stream_key, shape, cuts, low, high):
    def one(dim, parts):
        heights = jax.random.uniform(jax.random.fold_in(jax.random.fold_in(stream_key, 6), dim), (parts,), jnp.float32, low / len(cuts), high / len(cuts))
        return jnp.repeat(jnp.exp(heights), shape[dim] // parts).reshape((-1,) + (1,) * (len(shape) - dim - 1))

    factor_of = one(*cuts[0])
    for cut in cuts[1:]:
        factor_of = factor_of * one(*cut)
    return factor_of


def normal_values(key, shape, deviation, bound, pieces=(), dtype=jnp.bfloat16):
    factor_of = shard_levels(key, shape, pieces, -0.22, 0.18) if pieces else 1.0
    array = jax.random.normal(key, shape, jnp.float32) * deviation * factor_of
    return jnp.minimum(jnp.maximum(array, -bound), bound).astype(dtype)


def bell_draw_with(stream_key, extent, spread, reach, split, heavy, kind=jnp.bfloat16):
    result = spread * jax.random.normal(stream_key, extent, jnp.float32)
    if split:
        result = result * shard_levels(stream_key, extent, split, -0.22, 0.18)
    return jnp.clip(strengthened(result, jax.random.fold_in(stream_key, 3), *heavy), -reach, reach).astype(kind)


def setup_inputs(seed: int = 0) -> dict:
    keys = jax.random.split(jax.random.key(seed), 13)
    slope_up = bell_draw_with(keys[0], (REPLICAS, WIDTH, INNER), 0.1, 1.25, ((0, 32), (2, 16)), (0, 1, 32, 2.75), jnp.float32)
    slope_down = bell_draw_with(keys[1], (REPLICAS, INNER, WIDTH), 0.1, 1.25, ((0, 32), (1, 16)), (0, 2, 32, 2.75), jnp.float32)
    slope_norm = bell_draw_with(keys[2], (REPLICAS, WIDTH), 1.0, 12.0, ((0, 32),), (0, 1, 32, 2.75), jnp.float32)
    slope_bias = bell_draw_with(keys[3], (REPLICAS, WIDTH), 1.0, 12.0, ((0, 32),), (0, 1, 32, 2.75), jnp.float32)
    param_up = normal_values(keys[4], (WIDTH, INNER), WIDTH ** -0.5, 0.15625, ((0, 32), (1, 16)), jnp.float32)
    param_down = normal_values(keys[5], (INNER, WIDTH), INNER ** -0.5, 0.078125, ((0, 16), (1, 32)), jnp.float32)
    param_norm = jnp.clip(1.0 + 0.15 * jax.random.normal(keys[6], (WIDTH,), jnp.float32), 0.25, 1.75)
    param_bias = normal_values(keys[7], (WIDTH,), 0.5, 3.0, ((0, 32),), jnp.float32)
    state_up = normal_values(keys[8], (WIDTH, INNER), 0.3, 1.75, ((0, 32), (1, 16)), jnp.float32)
    state_down = normal_values(keys[9], (INNER, WIDTH), 0.3, 1.75, ((0, 16), (1, 32)), jnp.float32)
    state_norm = normal_values(keys[10], (WIDTH,), 0.3, 1.75, ((0, 32),), jnp.float32)
    state_bias = normal_values(keys[11], (WIDTH,), 0.3, 1.75, ((0, 32),), jnp.float32)
    return dict(slope_up=slope_up, slope_down=slope_down, slope_norm=slope_norm, slope_bias=slope_bias, param_up=param_up, param_down=param_down, param_norm=param_norm, param_bias=param_bias, state_up=state_up, state_down=state_down, state_norm=state_norm, state_bias=state_bias)


learn_rate = 0.1
hold_rate = 0.7


def reference(slope_up, slope_down, slope_norm, slope_bias, param_up, param_down, param_norm, param_bias, state_up, state_down, state_norm, state_bias):
    mean_up = jnp.sum(slope_up.astype(jnp.float32), axis=0) * REPLICAS ** -0.5
    mean_down = jnp.sum(slope_down.astype(jnp.float32), axis=0) * REPLICAS ** -0.5
    mean_norm = jnp.sum(slope_norm.astype(jnp.float32), axis=0) * REPLICAS ** -0.5
    mean_bias = jnp.sum(slope_bias.astype(jnp.float32), axis=0) * REPLICAS ** -0.5
    state_new_up = hold_rate * state_up + mean_up
    next_up = param_up - learn_rate * state_new_up
    state_new_down = hold_rate * state_down + mean_down
    next_down = param_down - learn_rate * state_new_down
    state_new_norm = hold_rate * state_norm + mean_norm
    next_norm = param_norm - learn_rate * state_new_norm
    state_new_bias = hold_rate * state_bias + mean_bias
    next_bias = param_bias - learn_rate * state_new_bias
    half_up = next_up.astype(jnp.bfloat16)
    half_down = next_down.astype(jnp.bfloat16)
    half_norm = next_norm.astype(jnp.bfloat16)
    half_bias = next_bias.astype(jnp.bfloat16)
    return half_up, half_down, half_norm, half_bias, next_up, next_down, next_norm, next_bias, state_new_up, state_new_down, state_new_norm, state_new_bias
```

```python
import functools

import jax
import jax.numpy as jnp
from jax import lax
from jax.experimental import pallas as pl
from jax.experimental.pallas import tpu as pltpu
from jax.sharding import Mesh
from jax.sharding import PartitionSpec as P

DP = ("dp_0", "dp_1", "dp_2")
CHIPS = ("dp_0", "dp_1")
CORE = "dp_2"

learn_rate = 0.1
hold_rate = 0.7

SHARE = 40
COLS = 320
FOLD = 24
ROWS = 2 * SHARE + FOLD
HALF = 64


def eye(rows, cols, period=None):
    row = lax.broadcasted_iota(jnp.int32, (rows, cols), 0)
    col = lax.broadcasted_iota(jnp.int32, (rows, cols), 1)
    same = row == col
    if period:
        same = same | (row + period == col)
    return same.astype(jnp.bfloat16)


def times_transposed(a, b):
    return lax.dot_general(a, b, (((1,), (1,)), ((), ())), preferred_element_type=jnp.float32)


def low_lanes(rows):
    return lax.broadcasted_iota(jnp.int32, (rows, 128), 1) < HALF


def packed(first, second, tail, corner):
    upper = jnp.concatenate([tail[FOLD:], corner], axis=0)
    return jnp.concatenate([first, second, jnp.where(low_lanes(FOLD), tail[:FOLD], upper)], axis=0)


def split_kernel(chips, small, core_ref, x_ref, *refs):
    if small:
        norm_ref, bias_ref, keep_ref, send_ref = refs
    else:
        keep_ref, send_ref = refs
    first_core = core_ref[0] == 0
    one = eye(128, 128)
    blocks = []
    for k in range(chips * 2 * SHARE // 128):
        x = x_ref[:, k * 128 : (k + 1) * 128].astype(jnp.bfloat16)
        tail = x[256:]
        blocks.append(
            [
                times_transposed(one, x[:128]),
                times_transposed(one, x[128:256]),
                times_transposed(one, jnp.concatenate([tail, tail], axis=0)),
            ]
        )
    first, second, tail = (jnp.concatenate([b[j] for b in blocks], axis=0) for j in range(3))
    if small:
        zeros = jnp.zeros((1, HALF), jnp.float32)
        line = [jnp.concatenate([zeros, ref[...], zeros], axis=1) for ref in (norm_ref, bias_ref)]
        lines = jnp.concatenate(line + [jnp.zeros((6, line[0].shape[1]), jnp.float32)], axis=0)
    for i in range(chips):
        pair = []
        for c in range(2):
            at = (2 * i + c) * SHARE
            corner = lines[:, at : at + 128] if small else jnp.zeros((8, 128), jnp.float32)
            rows = slice(at, at + SHARE)
            pair.append(packed(first[rows], second[rows], tail[rows], corner))
        keep_ref[i] = jnp.where(first_core, pair[0], pair[1]).astype(jnp.bfloat16)
        send_ref[i] = jnp.where(first_core, pair[1], pair[0]).astype(jnp.bfloat16)


def split(core, x, small=()):
    cols, width = x.shape
    chips = width // (2 * SHARE)
    steps = 1 if small else 2
    out = jax.ShapeDtypeStruct((chips, ROWS, 128), jnp.bfloat16)
    spec = pl.BlockSpec((chips // steps, ROWS, 128), lambda i: (i, 0, 0))
    return pl.pallas_call(
        functools.partial(split_kernel, chips // steps, bool(small)),
        grid=(steps,),
        in_specs=[
            pl.BlockSpec(memory_space=pltpu.SMEM),
            pl.BlockSpec((cols, width // steps), lambda i: (0, i)),
        ]
        + [pl.BlockSpec((1, width), lambda i: (0, 0)) for _ in small],
        out_specs=[spec, spec],
        out_shape=[out, out],
    )(core, x, *small)


def moved(total, state, param, rate):
    state_new = hold_rate * state + total * rate
    return state_new, param - learn_rate * state_new


def update_kernel(rate, small, got_ref, param_ref, state_ref, *refs):
    if small:
        small_param_ref, small_state_ref, half_ref, next_ref, new_ref, small_next_ref, small_new_ref = refs
    else:
        half_ref, next_ref, new_ref = refs
    total = jnp.sum(got_ref[...].astype(jnp.float32), axis=0)
    folded = total[2 * SHARE :]
    shifted = jnp.concatenate([folded[:, HALF:], folded[:, :HALF]], axis=1)
    tail = jnp.concatenate([folded[:FOLD, :HALF], shifted[: SHARE - FOLD, :HALF]], axis=0)
    mean = jnp.concatenate([total[:SHARE], total[SHARE : 2 * SHARE], tail], axis=1)
    new, nxt = moved(mean, state_ref[...], param_ref[...], rate)
    new_ref[...] = new
    next_ref[...] = nxt
    if small:
        small_new, small_next = moved(folded[SHARE - FOLD :], small_state_ref[...], small_param_ref[...], rate)
        small_new_ref[...] = small_new
        small_next_ref[...] = small_next
        corner = small_next
    else:
        corner = jnp.zeros((8, 128), jnp.float32)
    twice = jnp.concatenate([nxt[:, 256:], nxt[:, 256:]], axis=1)
    half = packed(nxt[:, :128], nxt[:, 128:256], twice, corner).astype(jnp.bfloat16)
    for i in range(half_ref.shape[0]):
        half_ref[i] = half


def update(rate, got, param, state, small=()):
    mat = jax.ShapeDtypeStruct(param.shape, jnp.float32)
    line = jax.ShapeDtypeStruct((8, 128), jnp.float32)
    return pl.pallas_call(
        functools.partial(update_kernel, rate, bool(small)),
        out_shape=[jax.ShapeDtypeStruct(got.shape, jnp.bfloat16), mat, mat] + [line, line] * bool(small),
    )(got, param, state, *small)


def join_kernel(chips, core_ref, mine_ref, other_ref, out_ref):
    first_core = core_ref[0] == 0
    low = low_lanes(FOLD)
    parts = [[], [], []]
    for i in range(chips):
        mine = mine_ref[i].astype(jnp.float32)
        other = other_ref[i].astype(jnp.float32)
        for block in (jnp.where(first_core, mine, other), jnp.where(first_core, other, mine)):
            tail = block[2 * SHARE :]
            upper = SHARE - FOLD
            parts[0].append(block[:SHARE])
            parts[1].append(block[SHARE : 2 * SHARE])
            parts[2].append(jnp.where(low, tail, 0.0))
            parts[2].append(jnp.where(low[:upper], 0.0, tail[:upper]))
    first, second, tail = (jnp.concatenate(p, axis=0).astype(jnp.bfloat16) for p in parts)
    one = eye(128, 128)
    out_ref[:128] = times_transposed(one, first).astype(jnp.bfloat16)
    out_ref[128:256] = times_transposed(one, second).astype(jnp.bfloat16)
    out_ref[256:] = times_transposed(eye(HALF, 128, HALF), tail).astype(jnp.bfloat16)


def join(core, mine, other):
    chips = mine.shape[0]
    width = chips * 2 * SHARE
    steps = 2
    spec = pl.BlockSpec((chips // steps, ROWS, 128), lambda i: (i, 0, 0))
    return pl.pallas_call(
        functools.partial(join_kernel, chips // steps),
        grid=(steps,),
        in_specs=[pl.BlockSpec(memory_space=pltpu.SMEM), spec, spec],
        out_specs=pl.BlockSpec((COLS, width // steps), lambda i: (0, i)),
        out_shape=jax.ShapeDtypeStruct((COLS, width), jnp.bfloat16),
    )(core, mine, other)


def swapped(x):
    return lax.ppermute(x, CORE, [(0, 1), (1, 0)])


def over_chips(x):
    return lax.all_to_all(x, CHIPS, 0, 0, tiled=True)


def lines_of(first, second):
    return jnp.pad(jnp.stack([first, second]), ((0, 6), (HALF, HALF - first.shape[0])))


def body(
    slope_up,
    slope_down,
    slope_norm,
    slope_bias,
    param_up,
    param_down,
    param_norm,
    param_bias,
    state_up,
    state_down,
    state_norm,
    state_bias,
):
    rate = lax.axis_size(DP) ** (-0.5)
    core = lax.axis_index(CORE).astype(jnp.int32).reshape(1)

    keep_down, send_down = split(core, slope_down[0], (slope_norm, slope_bias))
    keep_up, send_up = split(core, slope_up[0].T)
    sum_down = keep_down + swapped(send_down)
    sum_up = keep_up + swapped(send_up)
    got_down = over_chips(sum_down)
    got_up = over_chips(sum_up)
    small = (lines_of(param_norm, param_bias), lines_of(state_norm, state_bias))
    copies_down, next_down, new_down, next_lines, new_lines = update(
        rate, got_down, param_down.T, state_down.T, small
    )
    copies_up, next_up, new_up = update(rate, got_up, param_up, state_up)
    mine_down = over_chips(copies_down)
    mine_up = over_chips(copies_up)
    other_down = swapped(mine_down)
    other_up = swapped(mine_up)
    half_down = join(core, mine_down, other_down)
    half_up = join(core, mine_up, other_up).T

    def corner(blocks):
        return blocks[:, ROWS - 8 : ROWS - 6, HALF : HALF + SHARE]

    is_first = core[0] == 0
    mine, other = corner(mine_down), corner(other_down)
    zero, one = jnp.where(is_first, mine, other), jnp.where(is_first, other, mine)
    halves = jnp.stack([zero, one], axis=1)
    half_norm = halves[:, :, 0].reshape(-1)
    half_bias = halves[:, :, 1].reshape(-1)

    def line(lines, row):
        return lines[row, HALF : HALF + SHARE]

    return (
        half_up,
        half_down,
        half_norm,
        half_bias,
        next_up,
        next_down.T,
        line(next_lines, 0),
        line(next_lines, 1),
        new_up,
        new_down.T,
        line(new_lines, 0),
        line(new_lines, 1),
    )


def solution(mesh):
    torus = Mesh(mesh.devices.reshape(4, 4, 2, mesh.shape["tp"]), ("dp_0", "dp_1", "dp_2", "tp"))
    placed = (
        P(DP, None, "tp"),
        P(DP, "tp", None),
        P(DP, None),
        P(DP, None),
        P(DP, "tp"),
        P("tp", DP),
        P(DP),
        P(DP),
        P(DP, "tp"),
        P("tp", DP),
        P(DP),
        P(DP),
    )
    return jax.shard_map(
        body,
        mesh=torus,
        in_specs=placed,
        out_specs=(
            P(None, "tp"),
            P("tp", None),
            P(),
            P(),
            P(DP, "tp"),
            P("tp", DP),
            P(DP),
            P(DP),
            P(DP, "tp"),
            P("tp", DP),
            P(DP),
            P(DP),
        ),
        check_vma=False,
    )
```

```python
import functools

import jax
import jax.numpy as jnp
from jax import lax
from jax.experimental import pallas as pl
from jax.experimental.pallas import tpu as pltpu
from jax.sharding import Mesh
from jax.sharding import PartitionSpec as P

DP = ("dp_0", "dp_1", "dp_2")
CORE = "dp_2"

learn_rate = 0.1
hold_rate = 0.7

SHARE = 40
COLS = 320
WIDTH = 1280
FOLD = 24
ROWS = 2 * SHARE + FOLD
HALF = 64
TALL = COLS + 8
DEEP = 256
PIECES = 4

VMEM = pl.BlockSpec(memory_space=pltpu.VMEM)
SMEM = pl.BlockSpec(memory_space=pltpu.SMEM)
HBM = pl.BlockSpec(memory_space=pltpu.HBM)
ROOM = pltpu.CompilerParams(vmem_limit_bytes=8 * 2**20)
FIRST = pltpu.CompilerParams(vmem_limit_bytes=55500000)
SECOND = pltpu.CompilerParams(vmem_limit_bytes=55000000)


def eye(rows, cols, period=None):
    row = lax.broadcasted_iota(jnp.int32, (rows, cols), 0)
    col = lax.broadcasted_iota(jnp.int32, (rows, cols), 1)
    same = row == col
    if period:
        same = same | (row + period == col)
    return same.astype(jnp.float32).astype(jnp.bfloat16)


def times_transposed(a, b):
    return lax.dot_general(a, b, (((1,), (1,)), ((), ())), preferred_element_type=jnp.float32)


def low_lanes(rows):
    return lax.broadcasted_iota(jnp.int32, (rows, 128), 1) < HALF


def packed(first, second, tail, corner):
    upper = jnp.concatenate([tail[FOLD:], corner], axis=0)
    return jnp.concatenate([first, second, jnp.where(low_lanes(FOLD), tail[:FOLD], upper)], axis=0)


def pick_kernel(want_ref, up_ref, down_ref, norm_ref, bias_ref, out_ref, held, line, sems):
    step = COLS // PIECES

    def copies(matrix, vector):
        yield pltpu.make_async_copy(vector, line, sems.at[PIECES])
        for k in range(PIECES):
            rows = pl.ds(k * step, step)
            yield pltpu.make_async_copy(matrix.at[rows], held.at[rows], sems.at[k])

    up = want_ref[0] == 0

    @pl.when(up)
    def _():
        for copy in copies(up_ref, norm_ref):
            copy.start()

    @pl.when(jnp.logical_not(up))
    def _():
        for copy in copies(down_ref, bias_ref):
            copy.start()

    waits = list(copies(up_ref, norm_ref))
    waits[0].wait()
    out_ref[COLS:] = jnp.broadcast_to(line[...], (TALL - COLS, WIDTH)).astype(jnp.bfloat16)
    for k in range(PIECES):
        waits[k + 1].wait()
        rows = slice(k * step, (k + 1) * step)
        out_ref[rows] = held[rows].astype(jnp.bfloat16)


def pick(room, want, up, down, norm, bias):
    return pl.pallas_call(
        pick_kernel,
        in_specs=[SMEM, HBM, HBM, HBM, HBM],
        out_specs=VMEM,
        out_shape=jax.ShapeDtypeStruct((TALL, WIDTH), jnp.bfloat16),
        scratch_shapes=[
            pltpu.VMEM((COLS, WIDTH), jnp.float32),
            pltpu.VMEM((1, WIDTH), jnp.float32),
            pltpu.SemaphoreType.DMA((PIECES + 1,)),
        ],
        compiler_params=room,
        cost_estimate=pl.CostEstimate(flops=10**6, bytes_accessed=3 * 10**6, transcendentals=0),
    )(want, up, down, norm, bias)


def split_kernel(mine_ref, other_ref, out_ref, turned):
    one = eye(DEEP, DEEP)
    for k in range(WIDTH // DEEP):
        lanes = slice(k * DEEP, (k + 1) * DEEP)
        x = mine_ref[:COLS, lanes].astype(jnp.float32) + other_ref[:COLS, lanes].astype(jnp.float32)
        x = x.astype(jnp.bfloat16)
        x = jnp.concatenate([x, x[256:]], axis=0)
        turned[lanes] = times_transposed(one, x)
    line = mine_ref[COLS:].astype(jnp.float32) + other_ref[COLS:].astype(jnp.float32)
    zeros = jnp.zeros((8, HALF), jnp.float32)
    line = jnp.concatenate([zeros, line, zeros], axis=1)
    for d in range(WIDTH // SHARE):
        at = d * SHARE
        rows = slice(at, at + SHARE)
        out_ref[d] = packed(
            turned[rows, :128], turned[rows, 128:256], turned[rows, 256:], line[:, at : at + 128]
        ).astype(jnp.bfloat16)


def split(mine, other):
    return pl.pallas_call(
        split_kernel,
        in_specs=[VMEM, VMEM],
        out_specs=VMEM,
        out_shape=jax.ShapeDtypeStruct((WIDTH // SHARE, ROWS, 128), jnp.bfloat16),
        scratch_shapes=[pltpu.VMEM((WIDTH, 384), jnp.float32)],
        compiler_params=ROOM,
    )(mine, other)


def moved(total, state, param, rate):
    state_new = hold_rate * state + total * rate
    return state_new, param - learn_rate * state_new


def update_kernel(rate, got_ref, *refs):
    params, states, (half_ref, *nexts), news = refs[:4], refs[4:8], refs[8:13], refs[13:]
    halves, corner = [], jnp.zeros((8, 128), jnp.float32)
    row = lax.broadcasted_iota(jnp.int32, (8, 128), 0)
    gap = jnp.zeros((1, HALF), jnp.float32)
    for c in range(2):
        total = got_ref[c].astype(jnp.float32)
        for i in range(1, got_ref.shape[0] // 2):
            total += got_ref[2 * i + c].astype(jnp.float32)
        folded = total[2 * SHARE :]
        shifted = jnp.concatenate([folded[:, HALF:], folded[:, :HALF]], axis=1)
        tail = jnp.concatenate([folded[:FOLD, :HALF], shifted[: SHARE - FOLD, :HALF]], axis=0)
        mean = jnp.concatenate([total[:SHARE], total[SHARE : 2 * SHARE], tail], axis=1)
        new, nxt = moved(mean, states[c][...], params[c][...], rate)
        news[c][...] = new
        nexts[c][...] = nxt
        line = shifted[SHARE - FOLD : SHARE - FOLD + 1, :SHARE]
        new, line = moved(line, states[2 + c][...].reshape(1, SHARE), params[2 + c][...].reshape(1, SHARE), rate)
        news[2 + c][...] = new.reshape(SHARE)
        nexts[2 + c][...] = line.reshape(SHARE)
        line = jnp.concatenate([gap, line, gap[:, : HALF - SHARE]], axis=1)
        corner = jnp.where(row == c, jnp.broadcast_to(line, (8, 128)), corner)
        halves.append((nxt[:, :128], nxt[:, 128:256], jnp.concatenate([nxt[:, 256:], nxt[:, 256:]], axis=1)))
    halves = [packed(*half, corner).astype(jnp.bfloat16) for half in halves]
    for d in range(half_ref.shape[0]):
        half_ref[d] = halves[d % 2]


def update(rate, got, params, states):
    held = [jax.ShapeDtypeStruct(p.shape, jnp.float32) for p in params]
    return pl.pallas_call(
        functools.partial(update_kernel, rate),
        in_specs=[VMEM] * 9,
        out_specs=[VMEM] * 9,
        out_shape=[jax.ShapeDtypeStruct(got.shape, jnp.bfloat16), *held, *held],
        compiler_params=ROOM,
    )(got, *params, *states)


def put(ref, up_ref, down_ref, is_up, sem):
    @pl.when(is_up)
    def _():
        pltpu.make_async_copy(ref, up_ref, sem).start()

    @pl.when(jnp.logical_not(is_up))
    def _():
        pltpu.make_async_copy(ref, down_ref, sem).start()

    return pltpu.make_async_copy(ref, up_ref, sem)


def join_kernel(core_ref, blocks_ref, out_ref, lines_ref, up_ref, down_ref, wide, tails, sem):
    low = low_lanes(FOLD)
    upper = SHARE - FOLD
    pieces = []
    for d in range(WIDTH // SHARE):
        at = d * SHARE
        block = blocks_ref[d].astype(jnp.float32)
        wide[at : at + SHARE, :128] = block[:SHARE]
        wide[at : at + SHARE, 128:] = block[SHARE : 2 * SHARE]
        tail = block[2 * SHARE :]
        tails[at : at + FOLD] = jnp.where(low, tail, 0.0)
        tails[at + FOLD : at + SHARE] = jnp.where(low[:upper], 0.0, tail[:upper])
        pieces.append(tail[upper:, HALF : HALF + SHARE])
    one = eye(DEEP, DEEP)
    folded = eye(HALF, 128, HALF)
    for k in range(WIDTH // DEEP):
        lanes = slice(k * DEEP, (k + 1) * DEEP)
        out_ref[:256, lanes] = times_transposed(one, wide[lanes].astype(jnp.bfloat16)).astype(jnp.bfloat16)
        out_ref[256:, lanes] = times_transposed(folded, tails[lanes].astype(jnp.bfloat16)).astype(jnp.bfloat16)
    copy = put(out_ref, up_ref, down_ref, core_ref[0] == 0, sem)
    lines_ref[...] = jnp.concatenate(pieces, axis=1).astype(jnp.bfloat16)
    copy.wait()


def join(core, blocks):
    whole = jax.ShapeDtypeStruct((COLS, WIDTH), jnp.bfloat16)
    return pl.pallas_call(
        join_kernel,
        in_specs=[SMEM, VMEM],
        out_specs=[VMEM, VMEM, HBM, HBM],
        out_shape=[whole, jax.ShapeDtypeStruct((8, WIDTH), jnp.bfloat16), whole, whole],
        scratch_shapes=[
            pltpu.VMEM((WIDTH, 256), jnp.float32),
            pltpu.VMEM((WIDTH, 128), jnp.float32),
            pltpu.SemaphoreType.DMA,
        ],
        compiler_params=ROOM,
    )(core, blocks)


def place_kernel(core_ref, other_ref, up_in, down_in, up_ref, down_ref, sem):
    put(other_ref, up_ref, down_ref, core_ref[0] != 0, sem).wait()


def place(core, other, up, down):
    whole = jax.ShapeDtypeStruct((COLS, WIDTH), jnp.bfloat16)
    return pl.pallas_call(
        place_kernel,
        in_specs=[SMEM, VMEM, HBM, HBM],
        out_specs=[HBM, HBM],
        out_shape=[whole, whole],
        input_output_aliases={2: 0, 3: 1},
        scratch_shapes=[pltpu.SemaphoreType.DMA],
        compiler_params=ROOM,
    )(core, other, up, down)


def swapped(x):
    return lax.ppermute(x, CORE, [(0, 1), (1, 0)])


def exchanged(x):
    return lax.all_to_all(x, DP, 0, 0, tiled=True)


def body(
    slope_up,
    slope_down,
    slope_norm,
    slope_bias,
    param_up,
    param_down,
    param_norm,
    param_bias,
    state_up,
    state_down,
    state_norm,
    state_bias,
):
    rate = lax.axis_size(DP) ** (-0.5)
    core = lax.axis_index(CORE).astype(jnp.int32).reshape(1)
    slopes = (slope_up[0].T, slope_down[0], slope_norm, slope_bias)
    params = (param_up, param_down.T, param_norm, param_bias)
    states = (state_up, state_down.T, state_norm, state_bias)

    other = swapped(pick(FIRST, 1 - core, *slopes))
    mine = pick(SECOND, core, *slopes)
    half, *held = update(rate, exchanged(split(mine, other)), params, states)
    next_up, next_down, next_norm, next_bias, new_up, new_down, new_norm, new_bias = held
    mine, lines, up, down = join(core, exchanged(half))
    up, down = place(core, swapped(mine), up, down)
    return (
        up.T,
        down,
        lines[0],
        lines[1],
        next_up,
        next_down.T,
        next_norm,
        next_bias,
        new_up,
        new_down.T,
        new_norm,
        new_bias,
    )


def solution(mesh):
    torus = Mesh(mesh.devices.reshape(4, 4, 2, mesh.shape["tp"]), ("dp_0", "dp_1", "dp_2", "tp"))
    placed = (
        P(DP, None, "tp"),
        P(DP, "tp", None),
        P(DP, None),
        P(DP, None),
        P(DP, "tp"),
        P("tp", DP),
        P(DP),
        P(DP),
        P(DP, "tp"),
        P("tp", DP),
        P(DP),
        P(DP),
    )
    return jax.shard_map(
        body,
        mesh=torus,
        in_specs=placed,
        out_specs=(
            P(None, "tp"),
            P("tp", None),
            P(),
            P(),
            P(DP, "tp"),
            P("tp", DP),
            P(DP),
            P(DP),
            P(DP, "tp"),
            P("tp", DP),
            P(DP),
            P(DP),
        ),
        check_vma=False,
    )
```

```python
import functools

import jax
import jax.numpy as jnp
from jax import lax
from jax.experimental import pallas as pl
from jax.experimental.pallas import tpu as pltpu
from jax.sharding import Mesh
from jax.sharding import PartitionSpec as P

DP = ("dp_0", "dp_1", "dp_2")
CORE = "dp_2"

learn_rate = 0.1
hold_rate = 0.7

SHARE = 40
COLS = 320
WIDTH = 1280
FOLD = 24
ROWS = 2 * SHARE + FOLD
HALF = 64
DEEP = 256
PIECES = 4

VMEM = pl.BlockSpec(memory_space=pltpu.VMEM)
SMEM = pl.BlockSpec(memory_space=pltpu.SMEM)
HBM = pl.BlockSpec(memory_space=pltpu.HBM)
ROOM = pltpu.CompilerParams(vmem_limit_bytes=8 * 2**20)
FIRST = pltpu.CompilerParams(vmem_limit_bytes=55500000)
SECOND = pltpu.CompilerParams(vmem_limit_bytes=55000000)


def eye(rows, cols, period=None):
    row = lax.broadcasted_iota(jnp.int32, (rows, cols), 0)
    col = lax.broadcasted_iota(jnp.int32, (rows, cols), 1)
    same = row == col
    if period:
        same = same | (row + period == col)
    return same.astype(jnp.float32).astype(jnp.bfloat16)


def times_transposed(a, b):
    return lax.dot_general(a, b, (((1,), (1,)), ((), ())), preferred_element_type=jnp.float32)


def low_lanes(rows):
    return lax.broadcasted_iota(jnp.int32, (rows, 128), 1) < HALF


def packed(first, second, tail, corner):
    upper = jnp.concatenate([tail[FOLD:], corner], axis=0)
    return jnp.concatenate([first, second, jnp.where(low_lanes(FOLD), tail[:FOLD], upper)], axis=0)


def pick_kernel(want_ref, up_ref, down_ref, out_ref, held, sems):
    step = COLS // PIECES

    def copies(matrix):
        for k in range(PIECES):
            rows = pl.ds(k * step, step)
            yield pltpu.make_async_copy(matrix.at[rows], held.at[rows], sems.at[k])

    up = want_ref[0] == 0

    @pl.when(up)
    def _():
        for copy in copies(up_ref):
            copy.start()

    @pl.when(jnp.logical_not(up))
    def _():
        for copy in copies(down_ref):
            copy.start()

    for k, copy in enumerate(copies(up_ref)):
        copy.wait()
        rows = slice(k * step, (k + 1) * step)
        out_ref[rows] = held[rows].astype(jnp.bfloat16)


def pick(room, want, up, down):
    return pl.pallas_call(
        pick_kernel,
        in_specs=[SMEM, HBM, HBM],
        out_specs=VMEM,
        out_shape=jax.ShapeDtypeStruct((COLS, WIDTH), jnp.bfloat16),
        scratch_shapes=[pltpu.VMEM((COLS, WIDTH), jnp.float32), pltpu.SemaphoreType.DMA((PIECES,))],
        compiler_params=room,
        cost_estimate=pl.CostEstimate(flops=10**6, bytes_accessed=3 * 10**6, transcendentals=0),
    )(want, up, down)


def split_kernel(mine_ref, other_ref, norm_ref, bias_ref, out_ref, turned):
    one = eye(DEEP, DEEP)
    for k in range(WIDTH // DEEP):
        lanes = slice(k * DEEP, (k + 1) * DEEP)
        x = mine_ref[:, lanes].astype(jnp.float32) + other_ref[:, lanes].astype(jnp.float32)
        x = x.astype(jnp.bfloat16)
        x = jnp.concatenate([x, x[256:]], axis=0)
        turned[lanes] = times_transposed(one, x)
    first_row = lax.broadcasted_iota(jnp.int32, (8, WIDTH), 0) == 0
    line = jnp.where(
        first_row, jnp.broadcast_to(norm_ref[...], (8, WIDTH)), jnp.broadcast_to(bias_ref[...], (8, WIDTH))
    )
    zeros = jnp.zeros((8, HALF), jnp.float32)
    line = jnp.concatenate([zeros, line, zeros], axis=1)
    for d in range(WIDTH // SHARE):
        at = d * SHARE
        rows = slice(at, at + SHARE)
        out_ref[d] = packed(
            turned[rows, :128], turned[rows, 128:256], turned[rows, 256:], line[:, at : at + 128]
        ).astype(jnp.bfloat16)


def split(mine, other, norm, bias):
    return pl.pallas_call(
        split_kernel,
        in_specs=[VMEM] * 4,
        out_specs=VMEM,
        out_shape=jax.ShapeDtypeStruct((WIDTH // SHARE, ROWS, 128), jnp.bfloat16),
        scratch_shapes=[pltpu.VMEM((WIDTH, 384), jnp.float32)],
        compiler_params=ROOM,
    )(mine, other, norm, bias)


def moved(total, state, param, rate):
    state_new = hold_rate * state + total * rate
    return state_new, param - learn_rate * state_new


def update_kernel(rate, got_ref, *refs):
    params, states, (half_ref, *nexts), news = refs[:4], refs[4:8], refs[8:13], refs[13:]
    halves, lines = [], 0.0
    for c in range(2):
        total = got_ref[c].astype(jnp.float32)
        for i in range(1, got_ref.shape[0] // 2):
            total += got_ref[2 * i + c].astype(jnp.float32)
        folded = total[2 * SHARE :]
        shifted = jnp.concatenate([folded[:, HALF:], folded[:, :HALF]], axis=1)
        lines += shifted[SHARE - FOLD :]
        tail = jnp.concatenate([folded[:FOLD, :HALF], shifted[: SHARE - FOLD, :HALF]], axis=0)
        mean = jnp.concatenate([total[:SHARE], total[SHARE : 2 * SHARE], tail], axis=1)
        new, nxt = moved(mean, states[c][...], params[c][...], rate)
        news[c][...] = new
        nexts[c][...] = nxt
        halves.append((nxt[:, :128], nxt[:, 128:256], jnp.concatenate([nxt[:, 256:], nxt[:, 256:]], axis=1)))
    row = lax.broadcasted_iota(jnp.int32, (8, 128), 0)
    gap = jnp.zeros((1, HALF), jnp.float32)
    corner = jnp.zeros((8, 128), jnp.float32)
    for c in range(2):
        state, param = (refs[2 + c][...].reshape(1, SHARE) for refs in (states, params))
        new, line = moved(lines[c : c + 1, :SHARE], state, param, rate)
        news[2 + c][...] = new.reshape(SHARE)
        nexts[2 + c][...] = line.reshape(SHARE)
        line = jnp.concatenate([gap, line, gap[:, : HALF - SHARE]], axis=1)
        corner = jnp.where(row == c, jnp.broadcast_to(line, (8, 128)), corner)
    halves = [packed(*half, corner).astype(jnp.bfloat16) for half in halves]
    for d in range(half_ref.shape[0]):
        half_ref[d] = halves[d % 2]


def update(rate, got, params, states):
    held = [jax.ShapeDtypeStruct(p.shape, jnp.float32) for p in params]
    return pl.pallas_call(
        functools.partial(update_kernel, rate),
        in_specs=[VMEM] * 9,
        out_specs=[VMEM] * 9,
        out_shape=[jax.ShapeDtypeStruct(got.shape, jnp.bfloat16), *held, *held],
        compiler_params=ROOM,
    )(got, *params, *states)


def join_kernel(blocks_ref, out_ref, lines_ref, wide, tails):
    low = low_lanes(FOLD)
    upper = SHARE - FOLD
    pieces = []
    for d in range(WIDTH // SHARE):
        at = d * SHARE
        block = blocks_ref[d].astype(jnp.float32)
        wide[at : at + SHARE, :128] = block[:SHARE]
        wide[at : at + SHARE, 128:] = block[SHARE : 2 * SHARE]
        tail = block[2 * SHARE :]
        tails[at : at + FOLD] = jnp.where(low, tail, 0.0)
        tails[at + FOLD : at + SHARE] = jnp.where(low[:upper], 0.0, tail[:upper])
        pieces.append(tail[upper:, HALF : HALF + SHARE])
    one = eye(DEEP, DEEP)
    folded = eye(HALF, 128, HALF)
    for k in range(WIDTH // DEEP):
        lanes = slice(k * DEEP, (k + 1) * DEEP)
        out_ref[:256, lanes] = times_transposed(one, wide[lanes].astype(jnp.bfloat16)).astype(jnp.bfloat16)
        out_ref[256:, lanes] = times_transposed(folded, tails[lanes].astype(jnp.bfloat16)).astype(jnp.bfloat16)
    lines_ref[...] = jnp.concatenate(pieces, axis=1).astype(jnp.bfloat16)


def join(blocks):
    return pl.pallas_call(
        join_kernel,
        in_specs=[VMEM],
        out_specs=[VMEM, VMEM],
        out_shape=[
            jax.ShapeDtypeStruct((COLS, WIDTH), jnp.bfloat16),
            jax.ShapeDtypeStruct((8, WIDTH), jnp.bfloat16),
        ],
        scratch_shapes=[pltpu.VMEM((WIDTH, 256), jnp.float32), pltpu.VMEM((WIDTH, 128), jnp.float32)],
        compiler_params=ROOM,
    )(blocks)


def place_kernel(core_ref, ref, *refs):
    up_ref, down_ref, sems = refs[-3:]
    step = COLS // PIECES
    is_up = core_ref[0] == 0

    def copies(to):
        for k in range(PIECES):
            rows = pl.ds(k * step, step)
            yield pltpu.make_async_copy(ref.at[rows], to.at[rows], sems.at[k])

    @pl.when(is_up)
    def _():
        for copy in copies(up_ref):
            copy.start()

    @pl.when(jnp.logical_not(is_up))
    def _():
        for copy in copies(down_ref):
            copy.start()

    for copy in copies(up_ref):
        copy.wait()


def place(core, matrix, *held):
    whole = jax.ShapeDtypeStruct((COLS, WIDTH), jnp.bfloat16)
    return pl.pallas_call(
        place_kernel,
        in_specs=[SMEM, VMEM] + [HBM for _ in held],
        out_specs=[HBM, HBM],
        out_shape=[whole, whole],
        input_output_aliases={2: 0, 3: 1} if held else {},
        scratch_shapes=[pltpu.SemaphoreType.DMA((PIECES,))],
        compiler_params=ROOM,
        cost_estimate=pl.CostEstimate(flops=0, bytes_accessed=2 * 10**6, transcendentals=0),
    )(core, matrix, *held)


def swapped(x):
    return lax.ppermute(x, CORE, [(0, 1), (1, 0)])


def exchanged(x):
    return lax.all_to_all(x, DP, 0, 0, tiled=True)


def body(
    slope_up,
    slope_down,
    slope_norm,
    slope_bias,
    param_up,
    param_down,
    param_norm,
    param_bias,
    state_up,
    state_down,
    state_norm,
    state_bias,
):
    rate = lax.axis_size(DP) ** (-0.5)
    core = lax.axis_index(CORE).astype(jnp.int32).reshape(1)
    slopes = (slope_up[0].T, slope_down[0])
    params = (param_up, param_down.T, param_norm, param_bias)
    states = (state_up, state_down.T, state_norm, state_bias)

    other = swapped(pick(FIRST, 1 - core, *slopes))
    mine = pick(SECOND, core, *slopes)
    half, *held = update(rate, exchanged(split(mine, other, slope_norm, slope_bias)), params, states)
    next_up, next_down, next_norm, next_bias, new_up, new_down, new_norm, new_bias = held
    mine, lines = join(exchanged(half))
    up, down = place(1 - core, swapped(mine), *place(core, mine))
    return (
        up.T,
        down,
        lines[0],
        lines[1],
        next_up,
        next_down.T,
        next_norm,
        next_bias,
        new_up,
        new_down.T,
        new_norm,
        new_bias,
    )


def solution(mesh):
    torus = Mesh(mesh.devices.reshape(4, 4, 2, mesh.shape["tp"]), ("dp_0", "dp_1", "dp_2", "tp"))
    placed = (
        P(DP, None, "tp"),
        P(DP, "tp", None),
        P(DP, None),
        P(DP, None),
        P(DP, "tp"),
        P("tp", DP),
        P(DP),
        P(DP),
        P(DP, "tp"),
        P("tp", DP),
        P(DP),
        P(DP),
    )
    return jax.shard_map(
        body,
        mesh=torus,
        in_specs=placed,
        out_specs=(
            P(None, "tp"),
            P("tp", None),
            P(),
            P(),
            P(DP, "tp"),
            P("tp", DP),
            P(DP),
            P(DP),
            P(DP, "tp"),
            P("tp", DP),
            P(DP),
            P(DP),
        ),
        check_vma=False,
    )
```

```python
import functools

import jax
import jax.numpy as jnp
from jax import lax
from jax.experimental import pallas as pl
from jax.experimental.pallas import tpu as pltpu
from jax.sharding import Mesh
from jax.sharding import PartitionSpec as P

DP = ("dp_0", "dp_1", "dp_2")
CORE = "dp_2"

learn_rate = 0.1
hold_rate = 0.7

SHARE = 40
COLS = 320
WIDTH = 1280
FOLD = 24
ROWS = 2 * SHARE + FOLD
HALF = 64
DEEP = 256
PIECES = 4

VMEM = pl.BlockSpec(memory_space=pltpu.VMEM)
SMEM = pl.BlockSpec(memory_space=pltpu.SMEM)
HBM = pl.BlockSpec(memory_space=pltpu.HBM)
ROOM = pltpu.CompilerParams(vmem_limit_bytes=8 * 2**20)
FIRST = pltpu.CompilerParams(vmem_limit_bytes=55500000)
SECOND = pltpu.CompilerParams(vmem_limit_bytes=55000000)


def eye(rows, cols, period=None):
    row = lax.broadcasted_iota(jnp.int32, (rows, cols), 0)
    col = lax.broadcasted_iota(jnp.int32, (rows, cols), 1)
    same = row == col
    if period:
        same = same | (row + period == col)
    return same.astype(jnp.float32).astype(jnp.bfloat16)


def times_transposed(a, b):
    return lax.dot_general(a, b, (((1,), (1,)), ((), ())), preferred_element_type=jnp.float32)


def low_lanes(rows):
    return lax.broadcasted_iota(jnp.int32, (rows, 128), 1) < HALF


def packed(first, second, tail, corner):
    upper = jnp.concatenate([tail[FOLD:], corner], axis=0)
    return jnp.concatenate([first, second, jnp.where(low_lanes(FOLD), tail[:FOLD], upper)], axis=0)


def pick_kernel(want_ref, up_ref, down_ref, out_ref, held, sems):
    step = COLS // PIECES

    def copies(matrix):
        for k in range(PIECES):
            rows = pl.ds(k * step, step)
            yield pltpu.make_async_copy(matrix.at[rows], held.at[rows], sems.at[k])

    up = want_ref[0] == 0

    @pl.when(up)
    def _():
        for copy in copies(up_ref):
            copy.start()

    @pl.when(jnp.logical_not(up))
    def _():
        for copy in copies(down_ref):
            copy.start()

    for k, copy in enumerate(copies(up_ref)):
        copy.wait()
        rows = slice(k * step, (k + 1) * step)
        out_ref[rows] = held[rows].astype(jnp.bfloat16)


def pick(room, want, up, down):
    return pl.pallas_call(
        pick_kernel,
        in_specs=[SMEM, HBM, HBM],
        out_specs=VMEM,
        out_shape=jax.ShapeDtypeStruct((COLS, WIDTH), jnp.bfloat16),
        scratch_shapes=[pltpu.VMEM((COLS, WIDTH), jnp.float32), pltpu.SemaphoreType.DMA((PIECES,))],
        compiler_params=room,
        cost_estimate=pl.CostEstimate(flops=10**6, bytes_accessed=3 * 10**6, transcendentals=0),
    )(want, up, down)


def split_kernel(mine_ref, other_ref, norm_ref, bias_ref, out_ref, turned):
    one = eye(DEEP, DEEP)
    for k in range(WIDTH // DEEP):
        lanes = slice(k * DEEP, (k + 1) * DEEP)
        x = mine_ref[:, lanes].astype(jnp.float32) + other_ref[:, lanes].astype(jnp.float32)
        x = x.astype(jnp.bfloat16)
        x = jnp.concatenate([x, x[256:]], axis=0)
        turned[lanes] = times_transposed(one, x)
    first_row = lax.broadcasted_iota(jnp.int32, (8, WIDTH), 0) == 0
    line = jnp.where(
        first_row, jnp.broadcast_to(norm_ref[...], (8, WIDTH)), jnp.broadcast_to(bias_ref[...], (8, WIDTH))
    )
    zeros = jnp.zeros((8, HALF), jnp.float32)
    line = jnp.concatenate([zeros, line, zeros], axis=1)
    for d in range(WIDTH // SHARE):
        at = d * SHARE
        rows = slice(at, at + SHARE)
        out_ref[d] = packed(
            turned[rows, :128], turned[rows, 128:256], turned[rows, 256:], line[:, at : at + 128]
        ).astype(jnp.bfloat16)


def split(mine, other, norm, bias):
    return pl.pallas_call(
        split_kernel,
        in_specs=[VMEM] * 4,
        out_specs=VMEM,
        out_shape=jax.ShapeDtypeStruct((WIDTH // SHARE, ROWS, 128), jnp.bfloat16),
        scratch_shapes=[pltpu.VMEM((WIDTH, 384), jnp.float32)],
        compiler_params=ROOM,
    )(mine, other, norm, bias)


def moved(total, state, param, rate):
    state_new = hold_rate * state + total * rate
    return state_new, param - learn_rate * state_new


def update_kernel(rate, got_ref, *refs):
    params, states, (half_ref, *nexts), news = refs[:4], refs[4:8], refs[8:13], refs[13:]
    halves, lines = [], 0.0
    for c in range(2):
        total = got_ref[c].astype(jnp.float32)
        for i in range(1, got_ref.shape[0] // 2):
            total += got_ref[2 * i + c].astype(jnp.float32)
        folded = total[2 * SHARE :]
        shifted = jnp.concatenate([folded[:, HALF:], folded[:, :HALF]], axis=1)
        lines += shifted[SHARE - FOLD :]
        tail = jnp.concatenate([folded[:FOLD, :HALF], shifted[: SHARE - FOLD, :HALF]], axis=0)
        mean = jnp.concatenate([total[:SHARE], total[SHARE : 2 * SHARE], tail], axis=1)
        new, nxt = moved(mean, states[c][...], params[c][...], rate)
        news[c][...] = new
        nexts[c][...] = nxt
        halves.append((nxt[:, :128], nxt[:, 128:256], jnp.concatenate([nxt[:, 256:], nxt[:, 256:]], axis=1)))
    row = lax.broadcasted_iota(jnp.int32, (8, 128), 0)
    gap = jnp.zeros((1, HALF), jnp.float32)
    corner = jnp.zeros((8, 128), jnp.float32)
    for c in range(2):
        state, param = (refs[2 + c][...].reshape(1, SHARE) for refs in (states, params))
        new, line = moved(lines[c : c + 1, :SHARE], state, param, rate)
        news[2 + c][...] = new.reshape(SHARE)
        nexts[2 + c][...] = line.reshape(SHARE)
        line = jnp.concatenate([gap, line, gap[:, : HALF - SHARE]], axis=1)
        corner = jnp.where(row == c, jnp.broadcast_to(line, (8, 128)), corner)
    halves = [packed(*half, corner).astype(jnp.bfloat16) for half in halves]
    for d in range(half_ref.shape[0]):
        half_ref[d] = halves[d % 2]


def update(rate, got, params, states):
    held = [jax.ShapeDtypeStruct(p.shape, jnp.float32) for p in params]
    return pl.pallas_call(
        functools.partial(update_kernel, rate),
        in_specs=[VMEM] * 9,
        out_specs=[VMEM] * 9,
        out_shape=[jax.ShapeDtypeStruct(got.shape, jnp.bfloat16), *held, *held],
        compiler_params=ROOM,
    )(got, *params, *states)


def join_kernel(small, core_ref, blocks_ref, *refs):
    wide, tails, out, sems = refs[-4:]
    if small:
        held, (lines_ref, up_ref, down_ref), placed = refs[:small], refs[small : small + 3], refs[small + 3 : -4]
    else:
        up_ref, down_ref = refs[2:4]
        held, placed = (), ()
    writes = [pltpu.make_async_copy(h, p, sems.at[i]) for i, (h, p) in enumerate(zip(held, placed))]
    for write in writes:
        write.start()
    is_up = core_ref[0] == 0

    def copy(to, k):
        lanes = pl.ds(k * DEEP, DEEP)
        return pltpu.make_async_copy(out.at[:, lanes], to.at[:, lanes], sems.at[small + k])

    low = low_lanes(FOLD)
    upper = SHARE - FOLD
    pieces = []
    one = eye(DEEP, DEEP)
    folded = eye(HALF, 128, HALF)
    d = 0
    for k in range(WIDTH // DEEP):
        while d * SHARE < (k + 1) * DEEP:
            at = d * SHARE
            block = blocks_ref[d].astype(jnp.float32)
            wide[at : at + SHARE, :128] = block[:SHARE]
            wide[at : at + SHARE, 128:] = block[SHARE : 2 * SHARE]
            tail = block[2 * SHARE :]
            tails[at : at + FOLD] = jnp.where(low, tail, 0.0)
            tails[at + FOLD : at + SHARE] = jnp.where(low[:upper], 0.0, tail[:upper])
            if small:
                pieces.append(tail[upper:, HALF : HALF + SHARE])
            d += 1
        lanes = slice(k * DEEP, (k + 1) * DEEP)
        out[:256, lanes] = times_transposed(one, wide[lanes].astype(jnp.bfloat16)).astype(jnp.bfloat16)
        out[256:, lanes] = times_transposed(folded, tails[lanes].astype(jnp.bfloat16)).astype(jnp.bfloat16)

        @pl.when(is_up)
        def _():
            copy(up_ref, k).start()

        @pl.when(jnp.logical_not(is_up))
        def _():
            copy(down_ref, k).start()

    if small:
        lines_ref[...] = jnp.concatenate(pieces, axis=1).astype(jnp.bfloat16)
    for write in writes:
        write.wait()
    for k in range(WIDTH // DEEP):
        copy(up_ref, k).wait()


def join(core, blocks, small=(), begun=()):
    whole = jax.ShapeDtypeStruct((COLS, WIDTH), jnp.bfloat16)
    lines = jax.ShapeDtypeStruct((8, WIDTH), jnp.bfloat16)
    return pl.pallas_call(
        functools.partial(join_kernel, len(small)),
        in_specs=[SMEM, VMEM] + [VMEM for _ in small] + [HBM for _ in begun],
        out_specs=[VMEM for _ in small[:1]] + [HBM, HBM] + [HBM for _ in small],
        out_shape=[lines for _ in small[:1]]
        + [whole, whole]
        + [jax.ShapeDtypeStruct(x.shape, x.dtype) for x in small],
        input_output_aliases={2: 0, 3: 1} if begun else {},
        scratch_shapes=[
            pltpu.VMEM((WIDTH, 256), jnp.float32),
            pltpu.VMEM((WIDTH, 128), jnp.float32),
            pltpu.VMEM((COLS, WIDTH), jnp.bfloat16),
            pltpu.SemaphoreType.DMA((len(small) + WIDTH // DEEP,)),
        ],
        compiler_params=ROOM,
        cost_estimate=pl.CostEstimate(flops=10**9, bytes_accessed=2 * 10**6, transcendentals=0),
    )(core, blocks, *small, *begun)


def swapped(x):
    return lax.ppermute(x, CORE, [(0, 1), (1, 0)])


def exchanged(x):
    return lax.all_to_all(x, DP, 0, 0, tiled=True)


def body(
    slope_up,
    slope_down,
    slope_norm,
    slope_bias,
    param_up,
    param_down,
    param_norm,
    param_bias,
    state_up,
    state_down,
    state_norm,
    state_bias,
):
    rate = lax.axis_size(DP) ** (-0.5)
    core = lax.axis_index(CORE).astype(jnp.int32).reshape(1)
    slopes = (slope_up[0].T, slope_down[0])
    params = (param_up, param_down.T, param_norm, param_bias)
    states = (state_up, state_down.T, state_norm, state_bias)

    other = swapped(pick(FIRST, 1 - core, *slopes))
    mine = pick(SECOND, core, *slopes)
    half, *held = update(rate, exchanged(split(mine, other, slope_norm, slope_bias)), params, states)
    mine = exchanged(half)
    other = swapped(mine)
    lines, *begun, next_up, next_down, next_norm, next_bias, new_up, new_down, new_norm, new_bias = join(
        core, mine, held
    )
    up, down = join(1 - core, other, begun=begun)
    return (
        up.T,
        down,
        lines[0],
        lines[1],
        next_up,
        next_down.T,
        next_norm,
        next_bias,
        new_up,
        new_down.T,
        new_norm,
        new_bias,
    )


def solution(mesh):
    torus = Mesh(mesh.devices.reshape(4, 4, 2, mesh.shape["tp"]), ("dp_0", "dp_1", "dp_2", "tp"))
    placed = (
        P(DP, None, "tp"),
        P(DP, "tp", None),
        P(DP, None),
        P(DP, None),
        P(DP, "tp"),
        P("tp", DP),
        P(DP),
        P(DP),
        P(DP, "tp"),
        P("tp", DP),
        P(DP),
        P(DP),
    )
    return jax.shard_map(
        body,
        mesh=torus,
        in_specs=placed,
        out_specs=(
            P(None, "tp"),
            P("tp", None),
            P(),
            P(),
            P(DP, "tp"),
            P("tp", DP),
            P(DP),
            P(DP),
            P(DP, "tp"),
            P("tp", DP),
            P(DP),
            P(DP),
        ),
        check_vma=False,
    )
```

```python
import functools

import jax
import jax.numpy as jnp
from jax import lax
from jax.experimental import pallas as pl
from jax.experimental.pallas import tpu as pltpu
from jax.sharding import Mesh
from jax.sharding import PartitionSpec as P

DP = ("y_1", "y_0", "x_1", "x_0", "core")
CORE = "core"
GATHER = ("x_1", "x_0", "y_1", "y_0", "core")
SPREAD = ("y_1", "y_0", "x_1", "core", "x_0")

learn_rate = 0.1
hold_rate = 0.7

SHARE = 40
COLS = 320
WIDTH = 1280
FOLD = 24
ROWS = 2 * SHARE + FOLD
HALF = 64
DEEP = 256
PIECES = 4

VMEM = pl.BlockSpec(memory_space=pltpu.VMEM)
SMEM = pl.BlockSpec(memory_space=pltpu.SMEM)
HBM = pl.BlockSpec(memory_space=pltpu.HBM)
ROOM = pltpu.CompilerParams(vmem_limit_bytes=8 * 2**20)
FIRST = pltpu.CompilerParams(vmem_limit_bytes=55500000)
SECOND = pltpu.CompilerParams(vmem_limit_bytes=55000000)


def turn(owner, path):
    bits = {axis: owner >> (len(DP) - 1 - i) & 1 for i, axis in enumerate(DP)}
    place = 0
    for axis in path:
        place = 2 * place + bits[axis]
    return place


def eye(rows, cols, period=None):
    row = lax.broadcasted_iota(jnp.int32, (rows, cols), 0)
    col = lax.broadcasted_iota(jnp.int32, (rows, cols), 1)
    same = row == col
    if period:
        same = same | (row + period == col)
    return same.astype(jnp.float32).astype(jnp.bfloat16)


def times_transposed(a, b):
    return lax.dot_general(a, b, (((1,), (1,)), ((), ())), preferred_element_type=jnp.float32)


def low_lanes(rows):
    return lax.broadcasted_iota(jnp.int32, (rows, 128), 1) < HALF


def packed(first, second, tail, corner):
    upper = jnp.concatenate([tail[FOLD:], corner], axis=0)
    return jnp.concatenate([first, second, jnp.where(low_lanes(FOLD), tail[:FOLD], upper)], axis=0)


def pick_kernel(want_ref, up_ref, down_ref, out_ref, held, sems):
    step = COLS // PIECES

    def copies(matrix):
        for k in range(PIECES):
            rows = pl.ds(k * step, step)
            yield pltpu.make_async_copy(matrix.at[rows], held.at[rows], sems.at[k])

    up = want_ref[0] == 0

    @pl.when(up)
    def _():
        for copy in copies(up_ref):
            copy.start()

    @pl.when(jnp.logical_not(up))
    def _():
        for copy in copies(down_ref):
            copy.start()

    for k, copy in enumerate(copies(up_ref)):
        copy.wait()
        rows = slice(k * step, (k + 1) * step)
        out_ref[rows] = held[rows].astype(jnp.bfloat16)


def pick(room, want, up, down):
    return pl.pallas_call(
        pick_kernel,
        in_specs=[SMEM, HBM, HBM],
        out_specs=VMEM,
        out_shape=jax.ShapeDtypeStruct((COLS, WIDTH), jnp.bfloat16),
        scratch_shapes=[pltpu.VMEM((COLS, WIDTH), jnp.float32), pltpu.SemaphoreType.DMA((PIECES,))],
        compiler_params=room,
        cost_estimate=pl.CostEstimate(flops=10**6, bytes_accessed=3 * 10**6, transcendentals=0),
    )(want, up, down)


def split_kernel(mine_ref, other_ref, norm_ref, bias_ref, out_ref, turned):
    one = eye(DEEP, DEEP)
    for k in range(WIDTH // DEEP):
        lanes = slice(k * DEEP, (k + 1) * DEEP)
        x = mine_ref[:, lanes].astype(jnp.float32) + other_ref[:, lanes].astype(jnp.float32)
        x = x.astype(jnp.bfloat16)
        x = jnp.concatenate([x, x[256:]], axis=0)
        turned[lanes] = times_transposed(one, x)
    first_row = lax.broadcasted_iota(jnp.int32, (8, WIDTH), 0) == 0
    line = jnp.where(
        first_row, jnp.broadcast_to(norm_ref[...], (8, WIDTH)), jnp.broadcast_to(bias_ref[...], (8, WIDTH))
    )
    zeros = jnp.zeros((8, HALF), jnp.float32)
    line = jnp.concatenate([zeros, line, zeros], axis=1)
    for d in range(WIDTH // SHARE):
        at = d * SHARE
        rows = slice(at, at + SHARE)
        out_ref[turn(d, GATHER)] = packed(
            turned[rows, :128], turned[rows, 128:256], turned[rows, 256:], line[:, at : at + 128]
        ).astype(jnp.bfloat16)


def split(mine, other, norm, bias):
    return pl.pallas_call(
        split_kernel,
        in_specs=[VMEM] * 4,
        out_specs=VMEM,
        out_shape=jax.ShapeDtypeStruct((WIDTH // SHARE, ROWS, 128), jnp.bfloat16),
        scratch_shapes=[pltpu.VMEM((WIDTH, 384), jnp.float32)],
        compiler_params=ROOM,
    )(mine, other, norm, bias)


def moved(total, state, param, rate):
    state_new = hold_rate * state + total * rate
    return state_new, param - learn_rate * state_new


def update_kernel(rate, got_ref, *refs):
    params, states, (half_ref, *nexts), news = refs[:4], refs[4:8], refs[8:13], refs[13:]
    halves, lines = [], 0.0
    for c in range(2):
        total = got_ref[turn(c, GATHER)].astype(jnp.float32)
        for d in range(2 + c, got_ref.shape[0], 2):
            total += got_ref[turn(d, GATHER)].astype(jnp.float32)
        folded = total[2 * SHARE :]
        shifted = jnp.concatenate([folded[:, HALF:], folded[:, :HALF]], axis=1)
        lines += shifted[SHARE - FOLD :]
        tail = jnp.concatenate([folded[:FOLD, :HALF], shifted[: SHARE - FOLD, :HALF]], axis=0)
        mean = jnp.concatenate([total[:SHARE], total[SHARE : 2 * SHARE], tail], axis=1)
        new, nxt = moved(mean, states[c][...], params[c][...], rate)
        news[c][...] = new
        nexts[c][...] = nxt
        halves.append((nxt[:, :128], nxt[:, 128:256], jnp.concatenate([nxt[:, 256:], nxt[:, 256:]], axis=1)))
    row = lax.broadcasted_iota(jnp.int32, (8, 128), 0)
    gap = jnp.zeros((1, HALF), jnp.float32)
    corner = jnp.zeros((8, 128), jnp.float32)
    for c in range(2):
        state, param = (refs[2 + c][...].reshape(1, SHARE) for refs in (states, params))
        new, line = moved(lines[c : c + 1, :SHARE], state, param, rate)
        news[2 + c][...] = new.reshape(SHARE)
        nexts[2 + c][...] = line.reshape(SHARE)
        line = jnp.concatenate([gap, line, gap[:, : HALF - SHARE]], axis=1)
        corner = jnp.where(row == c, jnp.broadcast_to(line, (8, 128)), corner)
    halves = [packed(*half, corner).astype(jnp.bfloat16) for half in halves]
    for d in range(half_ref.shape[0]):
        half_ref[turn(d, SPREAD)] = halves[d % 2]


def update(rate, got, params, states):
    held = [jax.ShapeDtypeStruct(p.shape, jnp.float32) for p in params]
    return pl.pallas_call(
        functools.partial(update_kernel, rate),
        in_specs=[VMEM] * 9,
        out_specs=[VMEM] * 9,
        out_shape=[jax.ShapeDtypeStruct(got.shape, jnp.bfloat16), *held, *held],
        compiler_params=ROOM,
    )(got, *params, *states)


def join_kernel(small, core_ref, blocks_ref, *refs):
    wide, tails, out, sems = refs[-4:]
    if small:
        held, (lines_ref, up_ref, down_ref), placed = refs[:small], refs[small : small + 3], refs[small + 3 : -4]
    else:
        up_ref, down_ref = refs[2:4]
        held, placed = (), ()
    writes = [pltpu.make_async_copy(h, p, sems.at[i]) for i, (h, p) in enumerate(zip(held, placed))]
    for write in writes:
        write.start()
    is_up = core_ref[0] == 0

    def copy(to, k):
        lanes = pl.ds(k * DEEP, DEEP)
        return pltpu.make_async_copy(out.at[:, lanes], to.at[:, lanes], sems.at[small + k])

    low = low_lanes(FOLD)
    upper = SHARE - FOLD
    pieces = []
    one = eye(DEEP, DEEP)
    folded = eye(HALF, 128, HALF)
    d = 0
    for k in range(WIDTH // DEEP):
        while d * SHARE < (k + 1) * DEEP:
            at = d * SHARE
            block = blocks_ref[turn(d, SPREAD)].astype(jnp.float32)
            wide[at : at + SHARE, :128] = block[:SHARE]
            wide[at : at + SHARE, 128:] = block[SHARE : 2 * SHARE]
            tail = block[2 * SHARE :]
            tails[at : at + FOLD] = jnp.where(low, tail, 0.0)
            tails[at + FOLD : at + SHARE] = jnp.where(low[:upper], 0.0, tail[:upper])
            if small:
                pieces.append(tail[upper:, HALF : HALF + SHARE])
            d += 1
        lanes = slice(k * DEEP, (k + 1) * DEEP)
        out[:256, lanes] = times_transposed(one, wide[lanes].astype(jnp.bfloat16)).astype(jnp.bfloat16)
        out[256:, lanes] = times_transposed(folded, tails[lanes].astype(jnp.bfloat16)).astype(jnp.bfloat16)

        @pl.when(is_up)
        def _():
            copy(up_ref, k).start()

        @pl.when(jnp.logical_not(is_up))
        def _():
            copy(down_ref, k).start()

    if small:
        lines_ref[...] = jnp.concatenate(pieces, axis=1).astype(jnp.bfloat16)
    for write in writes:
        write.wait()
    for k in range(WIDTH // DEEP):
        copy(up_ref, k).wait()


def join(core, blocks, small=(), begun=()):
    whole = jax.ShapeDtypeStruct((COLS, WIDTH), jnp.bfloat16)
    lines = jax.ShapeDtypeStruct((8, WIDTH), jnp.bfloat16)
    return pl.pallas_call(
        functools.partial(join_kernel, len(small)),
        in_specs=[SMEM, VMEM] + [VMEM for _ in small] + [HBM for _ in begun],
        out_specs=[VMEM for _ in small[:1]] + [HBM, HBM] + [HBM for _ in small],
        out_shape=[lines for _ in small[:1]]
        + [whole, whole]
        + [jax.ShapeDtypeStruct(x.shape, x.dtype) for x in small],
        input_output_aliases={2: 0, 3: 1} if begun else {},
        scratch_shapes=[
            pltpu.VMEM((WIDTH, 256), jnp.float32),
            pltpu.VMEM((WIDTH, 128), jnp.float32),
            pltpu.VMEM((COLS, WIDTH), jnp.bfloat16),
            pltpu.SemaphoreType.DMA((len(small) + WIDTH // DEEP,)),
        ],
        compiler_params=ROOM,
        cost_estimate=pl.CostEstimate(flops=10**9, bytes_accessed=2 * 10**6, transcendentals=0),
    )(core, blocks, *small, *begun)


def swapped(x):
    return lax.ppermute(x, CORE, [(0, 1), (1, 0)])


def exchanged(x, path):
    return lax.all_to_all(x, path, 0, 0, tiled=True)


def body(
    slope_up,
    slope_down,
    slope_norm,
    slope_bias,
    param_up,
    param_down,
    param_norm,
    param_bias,
    state_up,
    state_down,
    state_norm,
    state_bias,
):
    rate = lax.axis_size(DP) ** (-0.5)
    core = lax.axis_index(CORE).astype(jnp.int32).reshape(1)
    slopes = (slope_up[0].T, slope_down[0])
    params = (param_up, param_down.T, param_norm, param_bias)
    states = (state_up, state_down.T, state_norm, state_bias)

    other = swapped(pick(FIRST, 1 - core, *slopes))
    mine = pick(SECOND, core, *slopes)
    half, *held = update(rate, exchanged(split(mine, other, slope_norm, slope_bias), GATHER), params, states)
    mine = exchanged(half, SPREAD)
    other = swapped(mine)
    lines, *begun, next_up, next_down, next_norm, next_bias, new_up, new_down, new_norm, new_bias = join(
        core, mine, held
    )
    up, down = join(1 - core, other, begun=begun)
    return (
        up.T,
        down,
        lines[0],
        lines[1],
        next_up,
        next_down.T,
        next_norm,
        next_bias,
        new_up,
        new_down.T,
        new_norm,
        new_bias,
    )


def solution(mesh):
    torus = Mesh(mesh.devices.reshape(2, 2, 2, 2, 2, mesh.shape["tp"]), (*DP, "tp"))
    placed = (
        P(DP, None, "tp"),
        P(DP, "tp", None),
        P(DP, None),
        P(DP, None),
        P(DP, "tp"),
        P("tp", DP),
        P(DP),
        P(DP),
        P(DP, "tp"),
        P("tp", DP),
        P(DP),
        P(DP),
    )
    return jax.shard_map(
        body,
        mesh=torus,
        in_specs=placed,
        out_specs=(
            P(None, "tp"),
            P("tp", None),
            P(),
            P(),
            P(DP, "tp"),
            P("tp", DP),
            P(DP),
            P(DP),
            P(DP, "tp"),
            P("tp", DP),
            P(DP),
            P(DP),
        ),
        check_vma=False,
    )
```

```python
import functools

import jax
import jax.numpy as jnp
from jax import lax
from jax.experimental import pallas as pl
from jax.experimental.pallas import tpu as pltpu
from jax.sharding import Mesh
from jax.sharding import PartitionSpec as P

DP = ("y_1", "y_0", "x_1", "x_0", "core")
CORE = "core"
GATHER = ("x_1", "x_0", "y_1", "y_0", "core")
SPREAD = ("y_1", "y_0", "x_1", "core", "x_0")

learn_rate = 0.1
hold_rate = 0.7

SHARE = 40
COLS = 320
WIDTH = 1280
FOLD = 24
ROWS = 2 * SHARE + FOLD
HALF = 64
DEEP = 256
PIECES = 4
BANDS = ((0, 128), (128, 128), (256, HALF))

VMEM = pl.BlockSpec(memory_space=pltpu.VMEM)
SMEM = pl.BlockSpec(memory_space=pltpu.SMEM)
HBM = pl.BlockSpec(memory_space=pltpu.HBM)
ROOM = pltpu.CompilerParams(vmem_limit_bytes=8 * 2**20)
FIRST = pltpu.CompilerParams(vmem_limit_bytes=55500000)
SECOND = pltpu.CompilerParams(vmem_limit_bytes=55000000)


def turn(owner, path):
    bits = {axis: owner >> (len(DP) - 1 - i) & 1 for i, axis in enumerate(DP)}
    place = 0
    for axis in path:
        place = 2 * place + bits[axis]
    return place


def eye(rows, cols, period=None):
    row = lax.broadcasted_iota(jnp.int32, (rows, cols), 0)
    col = lax.broadcasted_iota(jnp.int32, (rows, cols), 1)
    same = row == col
    if period:
        same = same | (row + period == col)
    return same.astype(jnp.float32).astype(jnp.bfloat16)


def times_transposed(a, b):
    return lax.dot_general(a, b, (((1,), (1,)), ((), ())), preferred_element_type=jnp.float32)


def low_lanes(rows):
    return lax.broadcasted_iota(jnp.int32, (rows, 128), 1) < HALF


def packed(first, second, tail, corner):
    upper = jnp.concatenate([tail[FOLD:], corner], axis=0)
    return jnp.concatenate([first, second, jnp.where(low_lanes(FOLD), tail[:FOLD], upper)], axis=0)


def pick_kernel(want_ref, up_ref, down_ref, out_ref, held, sems):
    step = COLS // PIECES

    def copies(matrix):
        for k in range(PIECES):
            rows = pl.ds(k * step, step)
            yield pltpu.make_async_copy(matrix.at[rows], held.at[rows], sems.at[k])

    up = want_ref[0] == 0

    @pl.when(up)
    def _():
        for copy in copies(up_ref):
            copy.start()

    @pl.when(jnp.logical_not(up))
    def _():
        for copy in copies(down_ref):
            copy.start()

    for k, copy in enumerate(copies(up_ref)):
        copy.wait()
        rows = slice(k * step, (k + 1) * step)
        out_ref[rows] = held[rows].astype(jnp.bfloat16)


def pick(room, want, up, down):
    return pl.pallas_call(
        pick_kernel,
        in_specs=[SMEM, HBM, HBM],
        out_specs=VMEM,
        out_shape=jax.ShapeDtypeStruct((COLS, WIDTH), jnp.bfloat16),
        scratch_shapes=[pltpu.VMEM((COLS, WIDTH), jnp.float32), pltpu.SemaphoreType.DMA((PIECES,))],
        compiler_params=room,
        cost_estimate=pl.CostEstimate(flops=10**6, bytes_accessed=3 * 10**6, transcendentals=0),
    )(want, up, down)


def split_kernel(mine_ref, other_ref, norm_ref, bias_ref, out_ref, turned):
    one = eye(DEEP, DEEP)
    for k in range(WIDTH // DEEP):
        lanes = slice(k * DEEP, (k + 1) * DEEP)
        x = mine_ref[:, lanes].astype(jnp.float32) + other_ref[:, lanes].astype(jnp.float32)
        x = x.astype(jnp.bfloat16)
        x = jnp.concatenate([x, x[256:]], axis=0)
        turned[lanes] = times_transposed(one, x)
    first_row = lax.broadcasted_iota(jnp.int32, (8, WIDTH), 0) == 0
    line = jnp.where(
        first_row, jnp.broadcast_to(norm_ref[...], (8, WIDTH)), jnp.broadcast_to(bias_ref[...], (8, WIDTH))
    )
    zeros = jnp.zeros((8, HALF), jnp.float32)
    line = jnp.concatenate([zeros, line, zeros], axis=1)
    for d in range(WIDTH // SHARE):
        at = d * SHARE
        rows = slice(at, at + SHARE)
        out_ref[turn(d, GATHER)] = packed(
            turned[rows, :128], turned[rows, 128:256], turned[rows, 256:], line[:, at : at + 128]
        ).astype(jnp.bfloat16)


def split(mine, other, norm, bias):
    return pl.pallas_call(
        split_kernel,
        in_specs=[VMEM] * 4,
        out_specs=VMEM,
        out_shape=jax.ShapeDtypeStruct((WIDTH // SHARE, ROWS, 128), jnp.bfloat16),
        scratch_shapes=[pltpu.VMEM((WIDTH, 384), jnp.float32)],
        compiler_params=ROOM,
    )(mine, other, norm, bias)


def moved(total, state, param, rate):
    state_new = hold_rate * state + total * rate
    return state_new, param - learn_rate * state_new


def update_kernel(rate, got_ref, *refs):
    params, states, (half_ref, *nexts), news = refs[:4], refs[4:8], refs[8:13], refs[13:]
    halves, lines = [], 0.0
    for c in range(2):
        total = got_ref[turn(c, GATHER)].astype(jnp.float32)
        for d in range(2 + c, got_ref.shape[0], 2):
            total += got_ref[turn(d, GATHER)].astype(jnp.float32)
        folded = total[2 * SHARE :]
        shifted = jnp.concatenate([folded[:, HALF:], folded[:, :HALF]], axis=1)
        lines += shifted[SHARE - FOLD :]
        tail = jnp.concatenate([folded[:FOLD, :HALF], shifted[: SHARE - FOLD, :HALF]], axis=0)
        mean = jnp.concatenate([total[:SHARE], total[SHARE : 2 * SHARE], tail], axis=1)
        new, nxt = moved(mean, states[c][...], params[c][...], rate)
        news[c][...] = new
        nexts[c][...] = nxt
        halves.append((nxt[:, :128], nxt[:, 128:256], jnp.concatenate([nxt[:, 256:], nxt[:, 256:]], axis=1)))
    row = lax.broadcasted_iota(jnp.int32, (8, 128), 0)
    gap = jnp.zeros((1, HALF), jnp.float32)
    corner = jnp.zeros((8, 128), jnp.float32)
    for c in range(2):
        state, param = (refs[2 + c][...].reshape(1, SHARE) for refs in (states, params))
        new, line = moved(lines[c : c + 1, :SHARE], state, param, rate)
        news[2 + c][...] = new.reshape(SHARE)
        nexts[2 + c][...] = line.reshape(SHARE)
        line = jnp.concatenate([gap, line, gap[:, : HALF - SHARE]], axis=1)
        corner = jnp.where(row == c, jnp.broadcast_to(line, (8, 128)), corner)
    halves = [packed(*half, corner).astype(jnp.bfloat16) for half in halves]
    for d in range(half_ref.shape[0]):
        half_ref[turn(d, SPREAD)] = halves[d % 2]


def update(rate, got, params, states):
    held = [jax.ShapeDtypeStruct(p.shape, jnp.float32) for p in params]
    return pl.pallas_call(
        functools.partial(update_kernel, rate),
        in_specs=[VMEM] * 9,
        out_specs=[VMEM] * 9,
        out_shape=[jax.ShapeDtypeStruct(got.shape, jnp.bfloat16), *held, *held],
        compiler_params=ROOM,
    )(got, *params, *states)


def join_kernel(small, core_ref, blocks_ref, *refs):
    wide, tails, out, sems = refs[-4:]
    if small:
        held, (lines_ref, up_ref, down_ref), placed = refs[:small], refs[small : small + 3], refs[small + 3 : -4]
    else:
        up_ref, down_ref = refs[2:4]
        held, placed = (), ()
    writes = [pltpu.make_async_copy(h, p, sems.at[i]) for i, (h, p) in enumerate(zip(held, placed))]
    for write in writes:
        write.start()
    is_up = core_ref[0] == 0

    def copy(to, k):
        rows = pl.ds(*BANDS[k])
        return pltpu.make_async_copy(out.at[rows], to.at[rows], sems.at[small + k])

    low = low_lanes(FOLD)
    upper = SHARE - FOLD
    pieces = []
    one = eye(128, 128)
    folded = eye(HALF, 128, HALF)
    for k, (first, many) in enumerate(BANDS):
        for d in range(WIDTH // SHARE):
            at = d * SHARE
            if many == HALF:
                tail = blocks_ref[turn(d, SPREAD), 2 * SHARE :].astype(jnp.float32)
                tails[at : at + FOLD] = jnp.where(low, tail, 0.0)
                tails[at + FOLD : at + SHARE] = jnp.where(low[:upper], 0.0, tail[:upper])
                if small:
                    pieces.append(tail[upper:, HALF : HALF + SHARE])
            else:
                rows = slice(first // 128 * SHARE, (first // 128 + 1) * SHARE)
                wide[at : at + SHARE, first : first + 128] = blocks_ref[turn(d, SPREAD), rows].astype(jnp.float32)
        for n in range(WIDTH // DEEP):
            lanes = slice(n * DEEP, (n + 1) * DEEP)
            if many == HALF:
                band = times_transposed(folded, tails[lanes].astype(jnp.bfloat16))
            else:
                band = times_transposed(one, wide[lanes, first : first + 128].astype(jnp.bfloat16))
            out[first : first + many, lanes] = band.astype(jnp.bfloat16)

        @pl.when(is_up)
        def _():
            copy(up_ref, k).start()

        @pl.when(jnp.logical_not(is_up))
        def _():
            copy(down_ref, k).start()

    if small:
        lines_ref[...] = jnp.concatenate(pieces, axis=1).astype(jnp.bfloat16)
    for write in writes:
        write.wait()
    for k in range(len(BANDS)):
        copy(up_ref, k).wait()


def join(core, blocks, small=(), begun=()):
    whole = jax.ShapeDtypeStruct((COLS, WIDTH), jnp.bfloat16)
    lines = jax.ShapeDtypeStruct((8, WIDTH), jnp.bfloat16)
    return pl.pallas_call(
        functools.partial(join_kernel, len(small)),
        in_specs=[SMEM, VMEM] + [VMEM for _ in small] + [HBM for _ in begun],
        out_specs=[VMEM for _ in small[:1]] + [HBM, HBM] + [HBM for _ in small],
        out_shape=[lines for _ in small[:1]]
        + [whole, whole]
        + [jax.ShapeDtypeStruct(x.shape, x.dtype) for x in small],
        input_output_aliases={2: 0, 3: 1} if begun else {},
        scratch_shapes=[
            pltpu.VMEM((WIDTH, 256), jnp.float32),
            pltpu.VMEM((WIDTH, 128), jnp.float32),
            pltpu.VMEM((COLS, WIDTH), jnp.bfloat16),
            pltpu.SemaphoreType.DMA((len(small) + len(BANDS),)),
        ],
        compiler_params=ROOM,
        cost_estimate=pl.CostEstimate(flops=10**9, bytes_accessed=2 * 10**6, transcendentals=0),
    )(core, blocks, *small, *begun)


def swapped(x):
    return lax.ppermute(x, CORE, [(0, 1), (1, 0)])


def exchanged(x, path):
    return lax.all_to_all(x, path, 0, 0, tiled=True)


def body(
    slope_up,
    slope_down,
    slope_norm,
    slope_bias,
    param_up,
    param_down,
    param_norm,
    param_bias,
    state_up,
    state_down,
    state_norm,
    state_bias,
):
    rate = lax.axis_size(DP) ** (-0.5)
    core = lax.axis_index(CORE).astype(jnp.int32).reshape(1)
    slopes = (slope_up[0].T, slope_down[0])
    params = (param_up, param_down.T, param_norm, param_bias)
    states = (state_up, state_down.T, state_norm, state_bias)

    other = swapped(pick(FIRST, 1 - core, *slopes))
    mine = pick(SECOND, core, *slopes)
    half, *held = update(rate, exchanged(split(mine, other, slope_norm, slope_bias), GATHER), params, states)
    mine = exchanged(half, SPREAD)
    other = swapped(mine)
    lines, *begun, next_up, next_down, next_norm, next_bias, new_up, new_down, new_norm, new_bias = join(
        core, mine, held
    )
    up, down = join(1 - core, other, begun=begun)
    return (
        up.T,
        down,
        lines[0],
        lines[1],
        next_up,
        next_down.T,
        next_norm,
        next_bias,
        new_up,
        new_down.T,
        new_norm,
        new_bias,
    )


def solution(mesh):
    torus = Mesh(mesh.devices.reshape(2, 2, 2, 2, 2, mesh.shape["tp"]), (*DP, "tp"))
    placed = (
        P(DP, None, "tp"),
        P(DP, "tp", None),
        P(DP, None),
        P(DP, None),
        P(DP, "tp"),
        P("tp", DP),
        P(DP),
        P(DP),
        P(DP, "tp"),
        P("tp", DP),
        P(DP),
        P(DP),
    )
    return jax.shard_map(
        body,
        mesh=torus,
        in_specs=placed,
        out_specs=(
            P(None, "tp"),
            P("tp", None),
            P(),
            P(),
            P(DP, "tp"),
            P("tp", DP),
            P(DP),
            P(DP),
            P(DP, "tp"),
            P("tp", DP),
            P(DP),
            P(DP),
        ),
        check_vma=False,
    )
```
